32 devices in a mesh: dp: 4 (over y, core), expert: 4 (over z), tensor: 2 (over x).
Axes of the slice: x: 2, y: 2, z: 4, core: 2. Of those that a mesh axis runs over, the one named last changes fastest.
Arguments:
- tokens: bfloat16 [256, 3072], P(('dp', 'expert')), may hold values from -45 to 45
- cotangent: bfloat16 [256, 3072], P(('dp', 'expert')), may hold values from -6 to 6
- gain: float32 [3072], replicated, may hold values from 0.5 to 1.5
- w_router: bfloat16 [3072, 4], replicated, may hold values from -0.109375 to 0.109375
- w_gate: bfloat16 [4, 3072, 9216], P('expert', None, 'tensor'), may hold values from -0.109375 to 0.109375
- w_up: bfloat16 [4, 3072, 9216], P('expert', None, 'tensor'), may hold values from -0.109375 to 0.109375
- w_down: bfloat16 [4, 9216, 3072], P('expert', 'tensor'), may hold values from -0.0625 to 0.0625
- expert_ids: int32 [256, 2], P(('dp', 'expert')), may hold values from 0 to 3, as said below
- slots: int32 [256, 2], P(('dp', 'expert')), may hold values from 0 to 7, as said below
Outputs:
- mixed: bfloat16 [256, 3072], P(('dp', 'expert'))
- grad_tokens: bfloat16 [256, 3072], P(('dp', 'expert'))
- grad_router: float32 [3072, 4], replicated
- grad_gain: float32 [3072], replicated
The draws below stay inside these ranges and needn't reach their ends.
Inputs may be any that keep to these rules, and one draw needn't show every extreme that they name: `expert_ids`: within each aligned block of 16 rows (one group), every expert is named exactly 8 times, and a row's two ids differ. Within each aligned block of 16 rows, the choices naming one expert hold its slots 0 to 7, each once.
All inputs are finite; a program needn't handle non-finite values.
Results may differ from the reference program's by a relative error of at most 0.0095.
Values may be sent and summed in bfloat16 or wider, within the bound.
A program may use at most 128 MiB of HBM per device.

```python
import jax
import jax.numpy as jnp
from jax import lax

D = 3072
FF = 9216
TOK_DEV = 16
SUBS = 1
EXPERTS = 4
CAP = 8
GROUPS = 16
TOKENS = 256


def draw_tokens(key, part):
    base_key, row_key, column_key = jax.random.split(key, 3)
    base = jax.random.truncated_normal(base_key, -4.0, 4.0, (TOKENS, D), jnp.float32)
    row_scale = 10.0 ** jax.random.uniform(row_key, (TOKENS, 1), jnp.float32, -0.5, 0.5)
    column_scale = 10.0 ** jax.random.uniform(column_key, (1, D), jnp.float32, -0.5, 0.5)
    return (base * row_scale * column_scale).astype(jnp.bfloat16)


def group_routes(group_key):
    perm_key, shift_key, swap_key, rank_key = jax.random.split(group_key, 4)
    shuffled = jax.random.permutation(perm_key, TOK_DEV).astype(jnp.int32)
    first_ids = shuffled % EXPERTS
    round_index = shuffled // EXPERTS
    shift_by = jax.random.randint(shift_key, (TOK_DEV // EXPERTS,), 1, EXPERTS).astype(jnp.int32)
    second_ids = (first_ids + shift_by[round_index]) % EXPERTS
    swapped = jax.random.randint(swap_key, (TOK_DEV,), 0, 2).astype(jnp.int32)
    left = jnp.where(swapped == 1, second_ids, first_ids)
    right = jnp.where(swapped == 1, first_ids, second_ids)
    chosen_ids = jnp.stack([left, right], axis=1)
    ranking = jax.random.permutation(rank_key, 2 * TOK_DEV).astype(jnp.int32)
    flat_ids = chosen_ids.reshape(-1)
    same_expert = flat_ids[:, None] == flat_ids[None, :]
    earlier = ranking[None, :] < ranking[:, None]
    slot_ids = jnp.sum((same_expert & earlier).astype(jnp.int32), axis=1).reshape(TOK_DEV, 2)
    return (chosen_ids, slot_ids)


def route_tables(key):
    folded = jax.random.fold_in(key, 7)
    group_keys = jax.random.split(folded, TOKENS // TOK_DEV)
    chosen_ids, slot_ids = jax.vmap(group_routes)(group_keys)
    return (chosen_ids.reshape(TOKENS, 2).astype(jnp.int32), slot_ids.reshape(TOKENS, 2).astype(jnp.int32))


def draw_expert_ids(key, part):
    return route_tables(key)[0]


def draw_slots(key, part):
    return route_tables(key)[1]


def levels(own_key, dims, pieces, low, top_value):
    loudness = 1.0
    for dim, parts in pieces:
        steps = jax.random.uniform(jax.random.fold_in(jax.random.fold_in(own_key, 6), dim), (parts,), jnp.float32, low / len(pieces), top_value / len(pieces))
        loudness = loudness * jnp.repeat(jnp.exp(steps), dims[dim] // parts).reshape((-1,) + (1,) * (len(dims) - 1 - dim))
    return loudness


def scatter_about(rng, dims, spread, bound, cuts=(), held_as=jnp.bfloat16):
    result = jax.random.normal(rng, dims, jnp.float32) * spread
    if len(cuts) > 0:
        result = levels(rng, dims, cuts, -0.22, 0.18) * result
    return jnp.clip(result, min=-bound, max=bound).astype(held_as)


def setup_inputs(seed: int = 0) -> dict:
    streams_of = jax.random.split(jax.random.key(seed), 10)
    tokens = draw_tokens(jax.random.fold_in(streams_of[9], 71), 0)
    cotangent = scatter_about(streams_of[1], (TOKENS, D), 1.0, 6.0, ((0, 16),))
    gain = jnp.clip(1.0 + 0.1 * jax.random.normal(streams_of[2], (D,), jnp.float32), 0.5, 1.5)
    w_router = scatter_about(streams_of[3], (D, EXPERTS), D ** -0.5, 0.109375)
    w_gate = scatter_about(streams_of[4], (EXPERTS * SUBS, D, FF // SUBS), D ** -0.5, 0.109375, ((0, 4), (2, 2)))
    w_up = scatter_about(streams_of[5], (EXPERTS * SUBS, D, FF // SUBS), D ** -0.5, 0.109375, ((0, 4), (2, 2)))
    w_down = scatter_about(streams_of[6], (EXPERTS * SUBS, FF // SUBS, D), FF ** -0.5, 0.0625, ((0, 4), (1, 2)))
    expert_ids = draw_expert_ids(jax.random.fold_in(streams_of[9], 71), 0)
    slots = draw_slots(jax.random.fold_in(streams_of[9], 71), 0)
    return {"tokens": tokens, "cotangent": cotangent, "gain": gain, "w_router": w_router, "w_gate": w_gate, "w_up": w_up, "w_down": w_down, "expert_ids": expert_ids, "slots": slots}


epsilon = 1e-05

def reference(tokens, cotangent, gain, w_router, w_gate, w_up, w_down, expert_ids, slots):
    floats = tokens.astype(jnp.float32)
    inv_rms = lax.rsqrt(lax.optimization_barrier(jnp.mean(floats * floats, axis=1, keepdims=True)) + epsilon)
    normed = (floats * inv_rms * gain).astype(jnp.bfloat16)
    logits = jnp.dot(normed, w_router, preferred_element_type=jnp.float32)
    chosen_logits = jnp.take_along_axis(logits, expert_ids, axis=1)
    first_prob = jax.nn.sigmoid(chosen_logits[:, 0] - chosen_logits[:, 1])
    pair_probs = jnp.stack([first_prob, 1.0 - first_prob], axis=1)
    feature_width = tokens.shape[1]
    group_index = jnp.arange(TOKENS, dtype=jnp.int32) // TOK_DEV
    places = (group_index[:, None] * CAP + slots).astype(jnp.int32)
    expert_inputs = jnp.zeros((EXPERTS, GROUPS * CAP, feature_width), jnp.bfloat16)
    expert_inputs = expert_inputs.at[expert_ids, places].set(jnp.broadcast_to(normed[:, None, :], (TOKENS, 2, feature_width)))
    upstream = cotangent.astype(jnp.float32)
    sent_grads = (pair_probs[:, :, None] * upstream[:, None, :]).astype(jnp.bfloat16)
    expert_grads = jnp.zeros((EXPERTS, GROUPS * CAP, feature_width), jnp.bfloat16)
    expert_grads = expert_grads.at[expert_ids, places].set(sent_grads)
    hidden = w_gate.shape[2]
    gate_blocks = w_gate.reshape(EXPERTS, SUBS, feature_width, hidden)
    up_blocks = w_up.reshape(EXPERTS, SUBS, feature_width, hidden)
    down_blocks = w_down.reshape(EXPERTS, SUBS * hidden, feature_width)

    def one_expert(operand):
        rows_in, grads_in, gate_part, up_part, down_full = operand
        gate_full = jnp.transpose(gate_part, (1, 0, 2)).reshape(feature_width, SUBS * hidden)
        up_full = jnp.transpose(up_part, (1, 0, 2)).reshape(feature_width, SUBS * hidden)
        gate_pre = jnp.dot(rows_in, gate_full, preferred_element_type=jnp.float32)
        up_pre = jnp.dot(rows_in, up_full, preferred_element_type=jnp.float32)
        activated = (jax.nn.silu(gate_pre) * up_pre).astype(jnp.bfloat16)
        expert_out = jnp.dot(activated, down_full, preferred_element_type=jnp.float32)
        grad_act = jnp.dot(grads_in, down_full.T, preferred_element_type=jnp.float32)
        sigmoid_gate = jax.nn.sigmoid(gate_pre)
        grad_gate = (grad_act * up_pre * sigmoid_gate * (1.0 + gate_pre * (1.0 - sigmoid_gate))).astype(jnp.bfloat16)
        grad_up = (grad_act * jax.nn.silu(gate_pre)).astype(jnp.bfloat16)
        expert_back = jnp.dot(grad_gate, gate_full.T, preferred_element_type=jnp.float32) + jnp.dot(grad_up, up_full.T, preferred_element_type=jnp.float32)
        return (expert_out, expert_back)
    expert_out, expert_back = lax.map(one_expert, (expert_inputs, expert_grads, gate_blocks, up_blocks, down_blocks))
    chosen = expert_out[expert_ids, places]
    mixed = (floats + lax.optimization_barrier(jnp.sum(pair_probs[:, :, None] * chosen, axis=1))).astype(jnp.bfloat16)
    grad_mixture = lax.optimization_barrier(jnp.sum(expert_back[expert_ids, places], axis=1))
    grad_probs = lax.optimization_barrier(jnp.sum(upstream[:, None, :] * chosen, axis=2))
    grad_first = first_prob * (1.0 - first_prob) * (grad_probs[:, 0] - grad_probs[:, 1])
    columns = jnp.arange(EXPERTS, dtype=jnp.int32)[None, :]
    grad_logits = grad_first[:, None] * ((expert_ids[:, 0:1] == columns).astype(jnp.float32) - (expert_ids[:, 1:2] == columns).astype(jnp.float32))
    grad_router = jnp.dot(normed.astype(jnp.float32).T, grad_logits, precision=lax.Precision.HIGHEST)
    grad_normed = grad_mixture + jnp.dot(grad_logits, w_router.astype(jnp.float32).T, precision=lax.Precision.HIGHEST)
    grad_gain = lax.optimization_barrier(jnp.sum(grad_normed * floats * inv_rms, axis=0))
    grad_scaled = grad_normed * gain
    cubed = inv_rms * inv_rms * inv_rms
    grad_tokens = (upstream + inv_rms * grad_scaled - floats * cubed * lax.optimization_barrier(jnp.mean(grad_scaled * floats, axis=1, keepdims=True))).astype(jnp.bfloat16)
    return (mixed, grad_tokens, grad_router, grad_gain)
```

```python
import functools

import jax
import jax.numpy as jnp
from jax import lax
from jax.experimental import pallas as pl
from jax.experimental.pallas import tpu as pltpu
from jax.sharding import PartitionSpec as P

epsilon = 1e-05


def pack_rows(select, values):
    return jnp.einsum("tcr,tcd->rd", select, values, preferred_element_type=jnp.float32).astype(
        jnp.bfloat16
    )


def repeat_blocks(packed, experts, copies):
    feature_width = packed.shape[1]
    blocks = packed.reshape(experts, 1, -1, feature_width)
    blocks = jnp.broadcast_to(blocks, (experts, copies, blocks.shape[2], feature_width))
    return blocks.reshape(experts * copies, -1, feature_width)


def to_experts(packed, experts, copies):
    arrived = lax.all_to_all(
        repeat_blocks(packed, experts, copies), "expert", split_axis=0, concat_axis=0, tiled=True
    )
    return arrived.reshape(-1, packed.shape[1])


def from_experts(partial_value, row_index, experts, copies):
    partial_value = lax.psum_scatter(
        partial_value.astype(jnp.bfloat16), "tensor", scatter_dimension=1, tiled=True
    ).astype(jnp.float32)
    feature_width = partial_value.shape[1]
    returned_rows = lax.all_to_all(
        partial_value.reshape(experts * copies, -1, feature_width),
        "expert",
        split_axis=0,
        concat_axis=0,
        tiled=True,
    )
    summed = jnp.sum(returned_rows.reshape(experts, copies, -1, feature_width), axis=1).reshape(
        -1, feature_width
    )
    picked = summed[row_index]
    picked = lax.all_gather(picked.astype(jnp.bfloat16), "tensor", axis=2, tiled=True).astype(
        picked.dtype
    )
    return picked


def shards(tokens, cotangent, gain, w_router, w_gate, w_up, w_down, expert_ids, slots):
    experts = w_router.shape[1]
    copies = lax.axis_size("expert") // experts
    token_count = tokens.shape[0]
    capacity = 2 * token_count // experts
    floats = tokens.astype(jnp.float32)
    inv_rms = lax.rsqrt(jnp.mean(floats * floats, axis=1, keepdims=True) + epsilon)
    normed = (floats * inv_rms * gain).astype(jnp.bfloat16)
    logits = jnp.dot(normed, w_router, preferred_element_type=jnp.float32)
    chosen_logits = jnp.take_along_axis(logits, expert_ids, axis=1)
    first_prob = jax.nn.sigmoid(chosen_logits[:, 0] - chosen_logits[:, 1])
    pair_probs = jnp.stack([first_prob, 1.0 - first_prob], axis=1)
    row_index = expert_ids * capacity + slots
    select = (
        row_index[:, :, None] == jnp.arange(experts * capacity, dtype=jnp.int32)[None, None, :]
    ).astype(jnp.bfloat16)
    feature_width = tokens.shape[1]
    inputs = to_experts(
        pack_rows(select, jnp.broadcast_to(normed[:, None, :], (token_count, 2, feature_width))),
        experts,
        copies,
    )
    gate_matrix = w_gate[0]
    up_matrix = w_up[0]
    down_matrix = w_down[0]
    gate_pre = jnp.dot(inputs, gate_matrix, preferred_element_type=jnp.float32)
    up_pre = jnp.dot(inputs, up_matrix, preferred_element_type=jnp.float32)
    activated = (jax.nn.silu(gate_pre) * up_pre).astype(jnp.bfloat16)
    chosen = from_experts(
        jnp.dot(activated, down_matrix, preferred_element_type=jnp.float32),
        row_index,
        experts,
        copies,
    )
    mixed = (floats + jnp.sum(pair_probs[:, :, None] * chosen, axis=1)).astype(jnp.bfloat16)
    upstream = cotangent.astype(jnp.float32)
    sent_grads = (pair_probs[:, :, None] * upstream[:, None, :]).astype(jnp.bfloat16)
    grad_outputs = to_experts(pack_rows(select, sent_grads), experts, copies)
    grad_act = jnp.dot(grad_outputs, down_matrix.T, preferred_element_type=jnp.float32)
    sigmoid_gate = jax.nn.sigmoid(gate_pre)
    grad_gate = (grad_act * up_pre * sigmoid_gate * (1.0 + gate_pre * (1.0 - sigmoid_gate))).astype(
        jnp.bfloat16
    )
    grad_up = (grad_act * jax.nn.silu(gate_pre)).astype(jnp.bfloat16)
    grad_inputs = jnp.dot(grad_gate, gate_matrix.T, preferred_element_type=jnp.float32) + jnp.dot(
        grad_up, up_matrix.T, preferred_element_type=jnp.float32
    )
    grad_mixture = jnp.sum(from_experts(grad_inputs, row_index, experts, copies), axis=1)
    grad_probs = jnp.sum(upstream[:, None, :] * chosen, axis=2)
    grad_first = first_prob * (1.0 - first_prob) * (grad_probs[:, 0] - grad_probs[:, 1])
    columns = jnp.arange(experts, dtype=jnp.int32)[None, :]
    grad_logits = grad_first[:, None] * (
        (expert_ids[:, 0:1] == columns).astype(jnp.float32)
        - (expert_ids[:, 1:2] == columns).astype(jnp.float32)
    )
    grad_normed = grad_mixture + jnp.dot(
        grad_logits, w_router.astype(jnp.float32).T, precision=lax.Precision.HIGHEST
    )
    router_part = jnp.dot(
        normed.astype(jnp.float32).T, grad_logits, precision=lax.Precision.HIGHEST
    )
    gain_part = jnp.sum(grad_normed * floats * inv_rms, axis=0)
    grad_router, grad_gain = lax.psum((router_part, gain_part), ("dp", "expert"))
    grad_scaled = grad_normed * gain
    cubed = inv_rms * inv_rms * inv_rms
    grad_tokens = (
        upstream
        + inv_rms * grad_scaled
        - floats * cubed * jnp.mean(grad_scaled * floats, axis=1, keepdims=True)
    ).astype(jnp.bfloat16)
    return (mixed, grad_tokens, grad_router, grad_gain)


def nt_dot(rows, matrix):
    return lax.dot_general(rows, matrix, (((1,), (1,)), ((), ())), preferred_element_type=jnp.float32)


def tn_dot(left, right):
    return lax.dot_general(left, right, (((0,), (0,)), ((), ())), preferred_element_type=jnp.float32)


def layer_kernel(
    E, NW, STEP,
    tok, cot, gain, router, ids, slots, wg_any, wu_any, wd_any,
    mixed_out, gtok_out, part_out,
    wg, wu, wd, w_sem,
    xsend, gsend, xbuf, gbuf, xs, gs,
    x_s, x_r, g_s, g_r, xf_s, xf_r, gf_s, gf_r,
    gate_s, up_s, act_s, gg_s, gu_s,
    yown, ybf, yrecv, yret, ybuf, ym_s, ym_r, yz_s, yz_r,
    iown, ibf, irecv, iret, ibuf, im_s, im_r, iz_s, iz_r,
    mxown, mxrecv, gdown, gdrecv, gmown, gmrecv, tx_s, tx_r,
):
    dp = lax.axis_index("dp")
    e = lax.axis_index("expert")
    t = lax.axis_index("tensor")
    c = lax.rem(dp, 2)
    mate = {"dp": dp + 1 - 2 * c}
    peer = {"tensor": 1 - t}
    tokens, D = tok.shape
    cap = xsend.shape[1]
    half = wg.shape[1]
    chunk = half // NW
    started = []

    def ahead(k):
        return lax.rem(e + k, E)

    def behind(k):
        return lax.rem(e + E - k, E)

    def send(src, dst, s, r, where):
        copy = pltpu.make_async_remote_copy(
            src_ref=src, dst_ref=dst, send_sem=s, recv_sem=r,
            device_id=where, device_id_type=pl.DeviceIdType.MESH,
        )
        copy.start()
        started.append(copy)
        return copy

    loads = []
    for kind, (src, dst) in enumerate(((wg_any, wg), (wu_any, wu), (wd_any, wd))):
        for i in range(NW):
            begin = pl.multiple_of(c * half + i * chunk, 128)
            here = pl.ds(i * chunk, chunk)
            if kind < 2:
                copy = pltpu.make_async_copy(
                    src.at[0, :, pl.ds(begin, chunk)], dst.at[:, here], w_sem.at[kind, i]
                )
            else:
                copy = pltpu.make_async_copy(
                    src.at[0, pl.ds(begin, chunk), :], dst.at[here, :], w_sem.at[kind, i]
                )
            loads.append(copy)
    for i in range(NW):
        loads[i].start()
        loads[NW + i].start()
    for i in range(NW):
        loads[2 * NW + i].start()

    barrier = pltpu.get_barrier_semaphore()
    for k in range(1, E):
        pl.semaphore_signal(
            barrier, inc=1, device_id={"expert": ahead(k)}, device_id_type=pl.DeviceIdType.MESH
        )
    pl.semaphore_signal(barrier, inc=1, device_id=mate, device_id_type=pl.DeviceIdType.MESH)
    pl.semaphore_signal(barrier, inc=1, device_id=peer, device_id_type=pl.DeviceIdType.MESH)

    floats = tok[...].astype(jnp.float32)
    inv = lax.rsqrt(jnp.mean(floats * floats, axis=1, keepdims=True) + epsilon)
    normed = (floats * inv * gain[...]).astype(jnp.bfloat16)
    place = ids[...] * cap + slots[...]
    lanes = lax.broadcasted_iota(jnp.int32, (tokens, E * cap), 1)
    sel0 = (place[:, 0:1] == lanes).astype(jnp.float32)
    sel1 = (place[:, 1:2] == lanes).astype(jnp.float32)
    both = (sel0 + sel1).astype(jnp.bfloat16)
    sel0 = sel0.astype(jnp.bfloat16)
    sel1 = sel1.astype(jnp.bfloat16)
    xsend[...] = tn_dot(both, normed).reshape(E, cap, D).astype(jnp.bfloat16)

    pl.semaphore_wait(barrier, E + 1)

    def dispatch(mine, buf, s, r, fs, fr):
        copies = [
            send(mine.at[ahead(k)], buf.at[c, e], s.at[k - 1], r.at[k - 1], {"expert": ahead(k)})
            for k in range(1, E)
        ]
        forwards = [send(mine.at[e], buf.at[c, e], fs.at[0], fr.at[0], mate)]
        buf[c, e] = mine[e]
        return copies, forwards

    def forward(copies, forwards, buf, fs, fr):
        for k in range(1, E):
            copies[k - 1].wait_recv()
            spot = buf.at[c, behind(k)]
            forwards.append(send(spot, spot, fs.at[k], fr.at[k], mate))

    def arrive(forwards, buf, rows):
        for copy in forwards:
            copy.wait_recv()
        rows[...] = buf[...].astype(jnp.float32).reshape(2 * E * cap, D).astype(jnp.bfloat16)

    x_copies, x_forwards = dispatch(xsend, xbuf, x_s, x_r, xf_s, xf_r)

    normed_f = normed.astype(jnp.float32)
    first, second = ids[:, 0:1], ids[:, 1:2]
    difference = jnp.zeros((tokens, 1), jnp.float32)
    for j in range(E):
        logit = jnp.sum(normed_f * router[j : j + 1, :].astype(jnp.float32), axis=1, keepdims=True)
        difference += jnp.where(first == j, logit, 0.0) - jnp.where(second == j, logit, 0.0)
    p0 = jax.nn.sigmoid(difference)
    p1 = 1.0 - p0
    upstream = cot[...].astype(jnp.float32)
    gsend[...] = (
        tn_dot(sel0, (p0 * upstream).astype(jnp.bfloat16))
        + tn_dot(sel1, (p1 * upstream).astype(jnp.bfloat16))
    ).reshape(E, cap, D).astype(jnp.bfloat16)
    g_copies, g_forwards = dispatch(gsend, gbuf, g_s, g_r, gf_s, gf_r)

    forward(x_copies, x_forwards, xbuf, xf_s, xf_r)
    arrive(x_forwards, xbuf, xs)

    per = chunk // STEP
    for i in range(NW):
        loads[i].wait()
        loads[NW + i].wait()

        @pl.loop(i * per, (i + 1) * per)
        def _(n):
            cols = pl.ds(pl.multiple_of(n * STEP, STEP), STEP)
            g = jnp.dot(xs[...], wg[:, cols], preferred_element_type=jnp.float32)
            u = jnp.dot(xs[...], wu[:, cols], preferred_element_type=jnp.float32)
            gate_s[:, cols] = g
            up_s[:, cols] = u
            act_s[:, cols] = (jax.nn.silu(g) * u).astype(jnp.bfloat16)

        if i == min(1, NW - 1):
            forward(g_copies, g_forwards, gbuf, gf_s, gf_r)

    for i in range(NW):
        loads[2 * NW + i].wait()

    @pl.loop(0, D // STEP)
    def _(n):
        cols = pl.ds(pl.multiple_of(n * STEP, STEP), STEP)
        y = jnp.dot(act_s[...], wd[:, cols], preferred_element_type=jnp.float32)
        y = y.reshape(2, E * cap, STEP)
        yown[:, :, cols] = y
        ybf[:, :, cols] = y.astype(jnp.bfloat16)

    y_mate = send(ybf.at[1 - c], yrecv, ym_s, ym_r, mate)
    arrive(g_forwards, gbuf, gs)

    def give_back(own, arrived, ret, buf, s, r):
        ret[...] = (own[c] + arrived[...].astype(jnp.float32)).reshape(E, cap, D).astype(jnp.bfloat16)
        copies = [
            send(ret.at[ahead(k)], buf.at[e], s.at[k - 1], r.at[k - 1], {"expert": ahead(k)})
            for k in range(1, E)
        ]
        buf[e] = ret[e]
        return copies

    def back_rows(copies, buf):
        for copy in copies:
            copy.wait_recv()
        return buf[...].astype(jnp.float32).reshape(E * cap, D).astype(jnp.bfloat16)

    for i in range(NW):

        @pl.loop(i * per, (i + 1) * per)
        def _(n):
            cols = pl.ds(pl.multiple_of(n * STEP, STEP), STEP)
            grad_act = nt_dot(gs[...], wd[cols, :])
            g = gate_s[:, cols]
            sig = jax.nn.sigmoid(g)
            gg_s[:, cols] = (grad_act * up_s[:, cols] * sig * (1.0 + g * (1.0 - sig))).astype(
                jnp.bfloat16
            )
            gu_s[:, cols] = (grad_act * (g * sig)).astype(jnp.bfloat16)

        if i == 0:
            y_mate.wait_recv()
            y_copies = give_back(yown, yrecv, yret, ybuf, yz_s, yz_r)

    rows = back_rows(y_copies, ybuf)
    chosen0 = jnp.dot(sel0, rows, preferred_element_type=jnp.float32)
    chosen1 = jnp.dot(sel1, rows, preferred_element_type=jnp.float32)
    mxown[...] = p0 * chosen0 + p1 * chosen1
    gdown[...] = jnp.broadcast_to(
        jnp.sum(upstream * (chosen0 - chosen1), axis=1, keepdims=True), gdown.shape
    )
    mx_copy = send(mxown, mxrecv, tx_s.at[0], tx_r.at[0], peer)
    gd_copy = send(gdown, gdrecv, tx_s.at[1], tx_r.at[1], peer)

    @pl.loop(0, D // STEP)
    def _(n):
        cols = pl.ds(pl.multiple_of(n * STEP, STEP), STEP)
        back = nt_dot(gg_s[...], wg[cols, :]) + nt_dot(gu_s[...], wu[cols, :])
        back = back.reshape(2, E * cap, STEP)
        iown[:, :, cols] = back
        ibf[:, :, cols] = back.astype(jnp.bfloat16)

    i_mate = send(ibf.at[1 - c], irecv, im_s, im_r, mate)

    mx_copy.wait_recv()
    gd_copy.wait_recv()
    mixed_out[...] = (floats + (mxown[...] + mxrecv[...])).astype(jnp.bfloat16)
    grad_first = p0 * (1.0 - p0) * (gdown[:, 0:1] + gdrecv[:, 0:1])
    part_out[...] = jnp.zeros_like(part_out)
    through_router = jnp.zeros((tokens, D), jnp.float32)
    for j in range(E):
        grad_logit = grad_first * ((first == j).astype(jnp.float32) - (second == j).astype(jnp.float32))
        through_router += grad_logit * router[j : j + 1, :].astype(jnp.float32)
        part_out[j : j + 1, :] = jnp.sum(grad_logit * normed_f, axis=0, keepdims=True)

    i_mate.wait_recv()
    i_copies = give_back(iown, irecv, iret, ibuf, iz_s, iz_r)
    rows = back_rows(i_copies, ibuf)
    gmown[...] = jnp.dot(both, rows, preferred_element_type=jnp.float32).astype(jnp.bfloat16)
    gm_copy = send(gmown, gmrecv, tx_s.at[2], tx_r.at[2], peer)
    gm_copy.wait_recv()
    grad_normed = (
        gmown[...].astype(jnp.float32) + gmrecv[...].astype(jnp.float32)
    ) + through_router
    part_out[E : E + 1, :] = jnp.sum(grad_normed * floats * inv, axis=0, keepdims=True)
    grad_scaled = grad_normed * gain[...]
    gtok_out[...] = (
        upstream
        + inv * grad_scaled
        - floats * (inv * inv * inv) * jnp.mean(grad_scaled * floats, axis=1, keepdims=True)
    ).astype(jnp.bfloat16)
    for copy in started:
        copy.wait_send()


def fused_shards(tokens, cotangent, gain, w_router, w_gate, w_up, w_down, expert_ids, slots):
    E = w_router.shape[1]
    count, D = tokens.shape
    cap = 2 * count // E
    half = w_gate.shape[2] // 2
    rows = E * cap
    bf, f32 = jnp.bfloat16, jnp.float32
    STEP = 256
    NW = 3 if half % (3 * STEP) == 0 else 1
    vmem, dma = pltpu.VMEM, pltpu.SemaphoreType.DMA
    whole = pl.BlockSpec(memory_space=pltpu.VMEM)
    back = [
        vmem((2, rows, D), f32), vmem((2, rows, D), bf), vmem((rows, D), bf),
        vmem((E, cap, D), bf), vmem((E, cap, D), bf),
        dma, dma, dma((E - 1,)), dma((E - 1,)),
    ]
    part_rows = -(-(E + 1) // 8) * 8
    mixed, grad_tokens, part = pl.pallas_call(
        functools.partial(layer_kernel, E, NW, STEP),
        out_shape=(
            jax.ShapeDtypeStruct((count, D), bf),
            jax.ShapeDtypeStruct((count, D), bf),
            jax.ShapeDtypeStruct((part_rows, D), f32),
        ),
        in_specs=[whole] * 6 + [pl.BlockSpec(memory_space=pl.ANY)] * 3,
        out_specs=(whole,) * 3,
        scratch_shapes=[
            vmem((D, half), bf), vmem((D, half), bf), vmem((half, D), bf), dma((3, NW)),
            vmem((E, cap, D), bf), vmem((E, cap, D), bf),
            vmem((2, E, cap, D), bf), vmem((2, E, cap, D), bf),
            vmem((2 * rows, D), bf), vmem((2 * rows, D), bf),
            dma((E - 1,)), dma((E - 1,)), dma((E - 1,)), dma((E - 1,)),
            dma((E,)), dma((E,)), dma((E,)), dma((E,)),
            vmem((2 * rows, half), f32), vmem((2 * rows, half), f32),
            vmem((2 * rows, half), bf), vmem((2 * rows, half), bf), vmem((2 * rows, half), bf),
            *back, *back,
            vmem((count, D), f32), vmem((count, D), f32),
            vmem((count, 128), f32), vmem((count, 128), f32),
            vmem((count, D), bf), vmem((count, D), bf),
            dma((3,)), dma((3,)),
        ],
        compiler_params=pltpu.CompilerParams(
            collective_id=0, has_side_effects=True, vmem_limit_bytes=63_000_000
        ),
    )(tokens, cotangent, gain[None, :], w_router.T, expert_ids, slots, w_gate, w_up, w_down)
    summed = lax.psum(part, ("dp", "expert"))
    return mixed, grad_tokens, summed[:E].T, summed[E]


def fits(mesh):
    return mesh.shape["dp"] % 2 == 0 and mesh.shape["tensor"] == 2 and mesh.shape["expert"] > 1


def shards_for(mesh):
    def body(*args):
        experts = args[3].shape[1]
        width, hidden = args[4].shape[1:]
        count = args[0].shape[0]
        cap = 2 * count // experts
        weights = 3 * width * hidden
        if (
            fits(mesh)
            and mesh.shape["expert"] == experts
            and hidden % 512 == 0
            and width % 256 == 0
            and cap % 8 == 0
            and weights <= 45_000_000
        ):
            return fused_shards(*args)
        return shards(*args)

    return body


def solution(mesh):
    return jax.shard_map(
        shards_for(mesh),
        mesh=mesh,
        in_specs=(
            P(("dp", "expert"), None),
            P(("dp", "expert"), None),
            P(),
            P(),
            P("expert", None, "tensor"),
            P("expert", None, "tensor"),
            P("expert", "tensor", None),
            P(("dp", "expert"), None),
            P(("dp", "expert"), None),
        ),
        out_specs=(P(("dp", "expert"), None), P(("dp", "expert"), None), P(), P()),
        check_vma=False,
    )
```

```python
import functools

import jax
import jax.numpy as jnp
from jax import lax
from jax.experimental import pallas as pl
from jax.experimental.pallas import tpu as pltpu
from jax.sharding import PartitionSpec as P

epsilon = 1e-05


def pack_rows(select, values):
    return jnp.einsum("tcr,tcd->rd", select, values, preferred_element_type=jnp.float32).astype(
        jnp.bfloat16
    )


def repeat_blocks(packed, experts, copies):
    feature_width = packed.shape[1]
    blocks = packed.reshape(experts, 1, -1, feature_width)
    blocks = jnp.broadcast_to(blocks, (experts, copies, blocks.shape[2], feature_width))
    return blocks.reshape(experts * copies, -1, feature_width)


def to_experts(packed, experts, copies):
    arrived = lax.all_to_all(
        repeat_blocks(packed, experts, copies), "expert", split_axis=0, concat_axis=0, tiled=True
    )
    return arrived.reshape(-1, packed.shape[1])


def from_experts(partial_value, row_index, experts, copies):
    partial_value = lax.psum_scatter(
        partial_value.astype(jnp.bfloat16), "tensor", scatter_dimension=1, tiled=True
    ).astype(jnp.float32)
    feature_width = partial_value.shape[1]
    returned_rows = lax.all_to_all(
        partial_value.reshape(experts * copies, -1, feature_width),
        "expert",
        split_axis=0,
        concat_axis=0,
        tiled=True,
    )
    summed = jnp.sum(returned_rows.reshape(experts, copies, -1, feature_width), axis=1).reshape(
        -1, feature_width
    )
    picked = summed[row_index]
    picked = lax.all_gather(picked.astype(jnp.bfloat16), "tensor", axis=2, tiled=True).astype(
        picked.dtype
    )
    return picked


def shards(tokens, cotangent, gain, w_router, w_gate, w_up, w_down, expert_ids, slots):
    experts = w_router.shape[1]
    copies = lax.axis_size("expert") // experts
    token_count = tokens.shape[0]
    capacity = 2 * token_count // experts
    floats = tokens.astype(jnp.float32)
    inv_rms = lax.rsqrt(jnp.mean(floats * floats, axis=1, keepdims=True) + epsilon)
    normed = (floats * inv_rms * gain).astype(jnp.bfloat16)
    logits = jnp.dot(normed, w_router, preferred_element_type=jnp.float32)
    chosen_logits = jnp.take_along_axis(logits, expert_ids, axis=1)
    first_prob = jax.nn.sigmoid(chosen_logits[:, 0] - chosen_logits[:, 1])
    pair_probs = jnp.stack([first_prob, 1.0 - first_prob], axis=1)
    row_index = expert_ids * capacity + slots
    select = (
        row_index[:, :, None] == jnp.arange(experts * capacity, dtype=jnp.int32)[None, None, :]
    ).astype(jnp.bfloat16)
    feature_width = tokens.shape[1]
    inputs = to_experts(
        pack_rows(select, jnp.broadcast_to(normed[:, None, :], (token_count, 2, feature_width))),
        experts,
        copies,
    )
    gate_matrix = w_gate[0]
    up_matrix = w_up[0]
    down_matrix = w_down[0]
    gate_pre = jnp.dot(inputs, gate_matrix, preferred_element_type=jnp.float32)
    up_pre = jnp.dot(inputs, up_matrix, preferred_element_type=jnp.float32)
    activated = (jax.nn.silu(gate_pre) * up_pre).astype(jnp.bfloat16)
    chosen = from_experts(
        jnp.dot(activated, down_matrix, preferred_element_type=jnp.float32),
        row_index,
        experts,
        copies,
    )
    mixed = (floats + jnp.sum(pair_probs[:, :, None] * chosen, axis=1)).astype(jnp.bfloat16)
    upstream = cotangent.astype(jnp.float32)
    sent_grads = (pair_probs[:, :, None] * upstream[:, None, :]).astype(jnp.bfloat16)
    grad_outputs = to_experts(pack_rows(select, sent_grads), experts, copies)
    grad_act = jnp.dot(grad_outputs, down_matrix.T, preferred_element_type=jnp.float32)
    sigmoid_gate = jax.nn.sigmoid(gate_pre)
    grad_gate = (grad_act * up_pre * sigmoid_gate * (1.0 + gate_pre * (1.0 - sigmoid_gate))).astype(
        jnp.bfloat16
    )
    grad_up = (grad_act * jax.nn.silu(gate_pre)).astype(jnp.bfloat16)
    grad_inputs = jnp.dot(grad_gate, gate_matrix.T, preferred_element_type=jnp.float32) + jnp.dot(
        grad_up, up_matrix.T, preferred_element_type=jnp.float32
    )
    grad_mixture = jnp.sum(from_experts(grad_inputs, row_index, experts, copies), axis=1)
    grad_probs = jnp.sum(upstream[:, None, :] * chosen, axis=2)
    grad_first = first_prob * (1.0 - first_prob) * (grad_probs[:, 0] - grad_probs[:, 1])
    columns = jnp.arange(experts, dtype=jnp.int32)[None, :]
    grad_logits = grad_first[:, None] * (
        (expert_ids[:, 0:1] == columns).astype(jnp.float32)
        - (expert_ids[:, 1:2] == columns).astype(jnp.float32)
    )
    grad_normed = grad_mixture + jnp.dot(
        grad_logits, w_router.astype(jnp.float32).T, precision=lax.Precision.HIGHEST
    )
    router_part = jnp.dot(
        normed.astype(jnp.float32).T, grad_logits, precision=lax.Precision.HIGHEST
    )
    gain_part = jnp.sum(grad_normed * floats * inv_rms, axis=0)
    grad_router, grad_gain = lax.psum((router_part, gain_part), ("dp", "expert"))
    grad_scaled = grad_normed * gain
    cubed = inv_rms * inv_rms * inv_rms
    grad_tokens = (
        upstream
        + inv_rms * grad_scaled
        - floats * cubed * jnp.mean(grad_scaled * floats, axis=1, keepdims=True)
    ).astype(jnp.bfloat16)
    return (mixed, grad_tokens, grad_router, grad_gain)


def nt_dot(rows, matrix):
    return lax.dot_general(rows, matrix, (((1,), (1,)), ((), ())), preferred_element_type=jnp.float32)


def tn_dot(left, right):
    return lax.dot_general(left, right, (((0,), (0,)), ((), ())), preferred_element_type=jnp.float32)


def layer_kernel(
    E, NW, STEP, NP, groups,
    tok, cot, gain, router, ids, slots, wg_any, wu_any, wd_any,
    mixed_out, gtok_out, part_out,
    wg, wu, wd, w_sem,
    xsend, gsend, xbuf, gbuf, xs, gs,
    x_s, x_r, g_s, g_r, xf_s, xf_r, gf_s, gf_r,
    gate_s, up_s, act_s, gg_s, gu_s,
    yown, ybf, yrecv, yret, ybuf, ym_s, ym_r, yz_s, yz_r,
    iown, ibf, irecv, iret, ibuf, im_s, im_r, iz_s, iz_r,
    mxown, mxrecv, gdown, gdrecv, gmown, gmrecv, tx_s, tx_r,
    blocks, inbox, outbox, rs_s, rs_r, ag_s, ag_r,
):
    dp = lax.axis_index("dp")
    e = lax.axis_index("expert")
    t = lax.axis_index("tensor")
    c = lax.rem(dp, 2)
    mate = {"dp": dp + 1 - 2 * c}
    peer = {"tensor": 1 - t}
    tokens, D = tok.shape
    cap = xsend.shape[1]
    half = wg.shape[1]
    chunk = half // NW
    started = []

    def ahead(k):
        return lax.rem(e + k, E)

    def behind(k):
        return lax.rem(e + E - k, E)

    def send(src, dst, s, r, where):
        copy = pltpu.make_async_remote_copy(
            src_ref=src, dst_ref=dst, send_sem=s, recv_sem=r,
            device_id=where, device_id_type=pl.DeviceIdType.MESH,
        )
        copy.start()
        started.append(copy)
        return copy

    loads = []
    for kind, (src, dst) in enumerate(((wg_any, wg), (wu_any, wu), (wd_any, wd))):
        for i in range(NW):
            begin = pl.multiple_of(c * half + i * chunk, 128)
            here = pl.ds(i * chunk, chunk)
            if kind < 2:
                copy = pltpu.make_async_copy(
                    src.at[0, :, pl.ds(begin, chunk)], dst.at[:, here], w_sem.at[kind, i]
                )
            else:
                copy = pltpu.make_async_copy(
                    src.at[0, pl.ds(begin, chunk), :], dst.at[here, :], w_sem.at[kind, i]
                )
            loads.append(copy)
    for i in range(NW):
        loads[i].start()
        loads[NW + i].start()
    for i in range(NW):
        loads[2 * NW + i].start()

    barrier = pltpu.get_barrier_semaphore()
    rank = dp * E + e

    def member(k):
        other = lax.rem(rank + k, groups)
        return other, {"dp": other // E, "expert": lax.rem(other, E)}

    for k in range(1, groups):
        pl.semaphore_signal(
            barrier, inc=1, device_id=member(k)[1], device_id_type=pl.DeviceIdType.MESH
        )
    pl.semaphore_signal(barrier, inc=1, device_id=peer, device_id_type=pl.DeviceIdType.MESH)

    floats = tok[...].astype(jnp.float32)
    inv = lax.rsqrt(jnp.mean(floats * floats, axis=1, keepdims=True) + epsilon)
    normed = (floats * inv * gain[...]).astype(jnp.bfloat16)
    place = ids[...] * cap + slots[...]
    index = lax.broadcasted_iota(jnp.int32, (E * cap, tokens), 0)
    sel0 = (place[0:1, :] == index).astype(jnp.float32)
    sel1 = (place[1:2, :] == index).astype(jnp.float32)
    both = (sel0 + sel1).astype(jnp.bfloat16)
    sel0 = sel0.astype(jnp.bfloat16)
    sel1 = sel1.astype(jnp.bfloat16)
    xsend[...] = jnp.dot(both, normed, preferred_element_type=jnp.float32).reshape(E, cap, D).astype(jnp.bfloat16)

    pl.semaphore_wait(barrier, groups)

    def dispatch(mine, buf, s, r, fs, fr):
        copies = [
            send(mine.at[ahead(k)], buf.at[c, e], s.at[k - 1], r.at[k - 1], {"expert": ahead(k)})
            for k in range(1, E)
        ]
        forwards = [send(mine.at[e], buf.at[c, e], fs.at[0], fr.at[0], mate)]
        buf[c, e] = mine[e]
        return copies, forwards

    def forward(copies, forwards, buf, fs, fr):
        for k in range(1, E):
            copies[k - 1].wait_recv()
            spot = buf.at[c, behind(k)]
            forwards.append(send(spot, spot, fs.at[k], fr.at[k], mate))

    def arrive(forwards, buf, rows):
        for copy in forwards:
            copy.wait_recv()
        rows[...] = buf[...].astype(jnp.float32).reshape(2 * E * cap, D).astype(jnp.bfloat16)

    x_copies, x_forwards = dispatch(xsend, xbuf, x_s, x_r, xf_s, xf_r)

    normed_f = normed.astype(jnp.float32)
    diagonal = lax.broadcasted_iota(jnp.int32, (tokens, tokens), 0) == lax.broadcasted_iota(
        jnp.int32, (tokens, tokens), 1
    )

    def as_column(row):
        return jnp.sum(jnp.where(diagonal, row.astype(jnp.float32), 0.0), axis=1, keepdims=True)

    first, second = as_column(ids[0:1, :]), as_column(ids[1:2, :])
    difference = jnp.zeros((tokens, 1), jnp.float32)
    for j in range(E):
        logit = jnp.sum(normed_f * router[j : j + 1, :].astype(jnp.float32), axis=1, keepdims=True)
        difference += jnp.where(first == j, logit, 0.0) - jnp.where(second == j, logit, 0.0)
    p0 = jax.nn.sigmoid(difference)
    p1 = 1.0 - p0
    upstream = cot[...].astype(jnp.float32)
    gsend[...] = (
        jnp.dot(sel0, (p0 * upstream).astype(jnp.bfloat16), preferred_element_type=jnp.float32)
        + jnp.dot(sel1, (p1 * upstream).astype(jnp.bfloat16), preferred_element_type=jnp.float32)
    ).reshape(E, cap, D).astype(jnp.bfloat16)
    g_copies, g_forwards = dispatch(gsend, gbuf, g_s, g_r, gf_s, gf_r)

    forward(x_copies, x_forwards, xbuf, xf_s, xf_r)
    arrive(x_forwards, xbuf, xs)

    per = chunk // STEP
    for i in range(NW):
        loads[i].wait()
        loads[NW + i].wait()

        @pl.loop(i * per, (i + 1) * per)
        def _(n):
            cols = pl.ds(pl.multiple_of(n * STEP, STEP), STEP)
            g = jnp.dot(xs[...], wg[:, cols], preferred_element_type=jnp.float32)
            u = jnp.dot(xs[...], wu[:, cols], preferred_element_type=jnp.float32)
            gate_s[:, cols] = g
            up_s[:, cols] = u
            act_s[:, cols] = (jax.nn.silu(g) * u).astype(jnp.bfloat16)

        if i == min(1, NW - 1):
            forward(g_copies, g_forwards, gbuf, gf_s, gf_r)

    for i in range(NW):
        loads[2 * NW + i].wait()

    @pl.loop(0, D // STEP)
    def _(n):
        cols = pl.ds(pl.multiple_of(n * STEP, STEP), STEP)
        y = jnp.dot(act_s[...], wd[:, cols], preferred_element_type=jnp.float32)
        y = y.reshape(2, E * cap, STEP)
        yown[:, :, cols] = y
        ybf[:, :, cols] = y.astype(jnp.bfloat16)

    y_mate = send(ybf.at[1 - c], yrecv, ym_s.at[0], ym_r.at[0], mate)
    arrive(g_forwards, gbuf, gs)

    def give_back(own, arrived, ret, buf, s, r, part, width):
        at = pl.ds(part * width, width)
        ret[:, :, at] = (own[c, :, at] + arrived[:, at].astype(jnp.float32)).reshape(
            E, cap, width
        ).astype(jnp.bfloat16)
        copies = [
            send(
                ret.at[ahead(k), :, at],
                buf.at[e, :, at],
                s.at[part, k - 1],
                r.at[part, k - 1],
                {"expert": ahead(k)},
            )
            for k in range(1, E)
        ]
        buf[e, :, at] = ret[e, :, at]
        return copies

    def back_rows(copies, buf):
        for copy in copies:
            copy.wait_recv()
        return buf[...].astype(jnp.float32).reshape(E * cap, D).astype(jnp.bfloat16)

    for i in range(NW):

        @pl.loop(i * per, (i + 1) * per)
        def _(n):
            cols = pl.ds(pl.multiple_of(n * STEP, STEP), STEP)
            grad_act = nt_dot(gs[...], wd[cols, :])
            g = gate_s[:, cols]
            sig = jax.nn.sigmoid(g)
            gg_s[:, cols] = (grad_act * up_s[:, cols] * sig * (1.0 + g * (1.0 - sig))).astype(
                jnp.bfloat16
            )
            gu_s[:, cols] = (grad_act * (g * sig)).astype(jnp.bfloat16)

        if i == 0:
            y_mate.wait_recv()
            y_copies = give_back(yown, yrecv, yret, ybuf, yz_s, yz_r, 0, D)

    rows = back_rows(y_copies, ybuf)
    chosen0 = tn_dot(sel0, rows)
    chosen1 = tn_dot(sel1, rows)
    mxown[...] = p0 * chosen0 + p1 * chosen1
    gdown[...] = jnp.broadcast_to(
        jnp.sum(upstream * (chosen0 - chosen1), axis=1, keepdims=True), gdown.shape
    )
    mx_copy = send(mxown, mxrecv, tx_s.at[0], tx_r.at[0], peer)
    gd_copy = send(gdown, gdrecv, tx_s.at[1], tx_r.at[1], peer)

    width = D // NP
    i_mates, i_copies = [], []

    def reduce_part(part):
        i_mates[part].wait_recv()
        i_copies.extend(give_back(iown, irecv, iret, ibuf, iz_s, iz_r, part, width))

    for part in range(NP):

        @pl.loop(part * (width // STEP), (part + 1) * (width // STEP))
        def _(n):
            cols = pl.ds(pl.multiple_of(n * STEP, STEP), STEP)
            back = nt_dot(gg_s[...], wg[cols, :]) + nt_dot(gu_s[...], wu[cols, :])
            back = back.reshape(2, E * cap, STEP)
            iown[:, :, cols] = back
            ibf[:, :, cols] = back.astype(jnp.bfloat16)

        at = pl.ds(part * width, width)
        i_mates.append(
            send(ibf.at[1 - c, :, at], irecv.at[:, at], im_s.at[part], im_r.at[part], mate)
        )
        if part > 0:
            reduce_part(part - 1)
    reduce_part(NP - 1)

    mx_copy.wait_recv()
    gd_copy.wait_recv()
    mixed_out[...] = (floats + (mxown[...] + mxrecv[...])).astype(jnp.bfloat16)
    grad_first = p0 * (1.0 - p0) * (gdown[:, 0:1] + gdrecv[:, 0:1])
    through_router = jnp.zeros((tokens, D), jnp.float32)
    sums = []
    for j in range(E):
        grad_logit = grad_first * ((first == j).astype(jnp.float32) - (second == j).astype(jnp.float32))
        through_router += grad_logit * router[j : j + 1, :].astype(jnp.float32)
        sums.append(jnp.sum(grad_logit * normed_f, axis=0, keepdims=True))

    rows = back_rows(i_copies, ibuf)
    gmown[...] = tn_dot(both, rows).astype(jnp.bfloat16)
    gm_copy = send(gmown, gmrecv, tx_s.at[2], tx_r.at[2], peer)
    gm_copy.wait_recv()
    grad_normed = (
        gmown[...].astype(jnp.float32) + gmrecv[...].astype(jnp.float32)
    ) + through_router
    sums.append(jnp.sum(grad_normed * floats * inv, axis=0, keepdims=True))
    piece = blocks.shape[2]
    blocks[...] = jnp.zeros_like(blocks)
    for j, row in enumerate(sums):
        for k in range(groups):
            blocks[k, j : j + 1, :] = row[:, k * piece : (k + 1) * piece]
    shares = []
    for k in range(1, groups):
        other, where = member(k)
        shares.append(send(blocks.at[other], inbox.at[rank], rs_s.at[k - 1], rs_r.at[k - 1], where))
    inbox[rank] = blocks[rank]
    grad_scaled = grad_normed * gain[...]
    gtok_out[...] = (
        upstream
        + inv * grad_scaled
        - floats * (inv * inv * inv) * jnp.mean(grad_scaled * floats, axis=1, keepdims=True)
    ).astype(jnp.bfloat16)
    for copy in shares:
        copy.wait_recv()
    total = inbox[0]
    for k in range(1, groups):
        total += inbox[k]
    outbox[rank] = total
    shares = []
    for k in range(1, groups):
        shares.append(
            send(outbox.at[rank], outbox.at[rank], ag_s.at[k - 1], ag_r.at[k - 1], member(k)[1])
        )
    for copy in shares:
        copy.wait_recv()
    for k in range(groups):
        part_out[:, k * piece : (k + 1) * piece] = outbox[k]
    for copy in started:
        copy.wait_send()


def unpack_kernel(E, mixed, gtok, part, mixed_out, gtok_out, router_out, gain_out):
    mixed_out[...] = mixed[...]
    gtok_out[...] = gtok[...]
    router_out[...] = part[0:E, :]
    gain_out[...] = part[E : E + 1, :]


def fused_shards(groups, tokens, cotangent, gain, w_router, w_gate, w_up, w_down, expert_ids, slots):
    E = w_router.shape[1]
    count, D = tokens.shape
    cap = 2 * count // E
    half = w_gate.shape[2] // 2
    rows = E * cap
    bf, f32 = jnp.bfloat16, jnp.float32
    STEP = 256
    NW = 3 if half % (3 * STEP) == 0 else 1
    NP = 3 if D % (3 * STEP) == 0 else 1
    vmem, dma = pltpu.VMEM, pltpu.SemaphoreType.DMA
    whole = pl.BlockSpec(memory_space=pltpu.VMEM)
    back = [
        vmem((2, rows, D), f32), vmem((2, rows, D), bf), vmem((rows, D), bf),
        vmem((E, cap, D), bf), vmem((E, cap, D), bf),
        dma((NP,)), dma((NP,)), dma((NP, E - 1)), dma((NP, E - 1)),
    ]
    part_rows = -(-(E + 1) // 8) * 8
    mixed, grad_tokens, part = pl.pallas_call(
        functools.partial(layer_kernel, E, NW, STEP, NP, groups),
        out_shape=(
            jax.ShapeDtypeStruct((count, D), bf),
            jax.ShapeDtypeStruct((count, D), bf),
            jax.ShapeDtypeStruct((part_rows, D), f32),
        ),
        in_specs=[whole] * 6 + [pl.BlockSpec(memory_space=pl.ANY)] * 3,
        out_specs=(whole,) * 3,
        scratch_shapes=[
            vmem((D, half), bf), vmem((D, half), bf), vmem((half, D), bf), dma((3, NW)),
            vmem((E, cap, D), bf), vmem((E, cap, D), bf),
            vmem((2, E, cap, D), bf), vmem((2, E, cap, D), bf),
            vmem((2 * rows, D), bf), vmem((2 * rows, D), bf),
            dma((E - 1,)), dma((E - 1,)), dma((E - 1,)), dma((E - 1,)),
            dma((E,)), dma((E,)), dma((E,)), dma((E,)),
            vmem((2 * rows, half), f32), vmem((2 * rows, half), f32),
            vmem((2 * rows, half), bf), vmem((2 * rows, half), bf), vmem((2 * rows, half), bf),
            *back, *back,
            vmem((count, D), f32), vmem((count, D), f32),
            vmem((count, 128), f32), vmem((count, 128), f32),
            vmem((count, D), bf), vmem((count, D), bf),
            dma((3,)), dma((3,)),
            *[vmem((groups, part_rows, D // groups), f32)] * 3,
            *[dma((groups - 1,))] * 4,
        ],
        compiler_params=pltpu.CompilerParams(
            collective_id=0, has_side_effects=True, vmem_limit_bytes=63_000_000
        ),
    )(tokens, cotangent, gain[None, :], w_router.T, expert_ids.T, slots.T, w_gate, w_up, w_down)
    mixed, grad_tokens, router, gain = pl.pallas_call(
        functools.partial(unpack_kernel, E),
        out_shape=(
            jax.ShapeDtypeStruct((count, D), bf),
            jax.ShapeDtypeStruct((count, D), bf),
            jax.ShapeDtypeStruct((E, D), f32),
            jax.ShapeDtypeStruct((1, D), f32),
        ),
        in_specs=[whole] * 3,
        out_specs=(whole,) * 4,
    )(mixed, grad_tokens, part)
    return mixed, grad_tokens, router.T, gain[0]


def fits(mesh):
    return mesh.shape["dp"] % 2 == 0 and mesh.shape["tensor"] == 2 and mesh.shape["expert"] > 1


def shards_for(mesh):
    def body(*args):
        experts = args[3].shape[1]
        width, hidden = args[4].shape[1:]
        count = args[0].shape[0]
        cap = 2 * count // experts
        weights = 3 * width * hidden
        if (
            fits(mesh)
            and mesh.shape["expert"] == experts
            and hidden % 512 == 0
            and width % 256 == 0
            and cap % 8 == 0
            and width % (mesh.shape["dp"] * experts) == 0
            and weights <= 45_000_000
        ):
            return fused_shards(mesh.shape["dp"] * experts, *args)
        return shards(*args)

    return body


def solution(mesh):
    return jax.shard_map(
        shards_for(mesh),
        mesh=mesh,
        in_specs=(
            P(("dp", "expert"), None),
            P(("dp", "expert"), None),
            P(),
            P(),
            P("expert", None, "tensor"),
            P("expert", None, "tensor"),
            P("expert", "tensor", None),
            P(("dp", "expert"), None),
            P(("dp", "expert"), None),
        ),
        out_specs=(P(("dp", "expert"), None), P(("dp", "expert"), None), P(), P()),
        check_vma=False,
    )
```
